32 devices in a mesh: member: 2 (over y), lon: 8 (over z, x), lat: 2 (over core).
Axes of the slice: x: 2, y: 2, z: 4, core: 2. Of those that a mesh axis runs over, the one named last changes fastest.
Arguments:
- state_tokens: bfloat16 [8, 24, 96, 768], P('member', 'lat', 'lon'), parts along dimension 0, may hold values from -32 to 32
- land_mask: int32 [24, 96], P('lat', 'lon'), may hold values 0 or 1
- pad_mask: int32 [24], replicated, may hold values from 0 to 1, as said below
- land_embed: float32 [2, 768], replicated, may hold values from -3 to 3
- w_qkv: bfloat16 [768, 1152], replicated, may hold values from -0.21875 to 0.21875
- w_proj: bfloat16 [384, 768], replicated, may hold values from -0.3125 to 0.3125
- proj_bias: float32 [768], replicated, may hold values from -4 to 4
- norm_gain: float32 [768], replicated, may hold values from 0.5 to 1.5
- norm_shift: float32 [768], replicated, may hold values from -1.5 to 1.5
- bias_table: bfloat16 [4, 2, 12, 3312], P('lat'), may hold values from -3.5 to 320
- index_table: int32 [144, 144], replicated, may hold values from 0 to 3311
Outputs:
- result: bfloat16 [8, 24, 96, 768], P('member', 'lat', 'lon'), parts along dimension 0
The draws below stay inside these ranges and needn't reach their ends.
There are 2 independent parts, one for each index of `member`. The reference program is written for one: setup_inputs(seed, part) draws one part's arguments, and reference() takes and returns one part's arrays. A program takes and returns all parts, laid end to end along the dimension named above; an argument that names none is the same for every part. Nothing has to cross between parts.
Inputs may be any that keep to these rules, and one draw needn't show every extreme that they name: pad_mask is 1 on every row except at most the first 2 and the last 2 of the 24 rows, which are 0 where padded; one of the two ends has exactly 2 padding rows.
All inputs are finite; a program needn't handle non-finite values. No bound on the sum of `land_mask` on one device may be relied on, other than what follows from the above.
Results may differ from the reference program's by a relative error of at most 0.0085.
Values may be sent and summed in bfloat16 or wider, within the bound.
A program may use at most 64 MiB of HBM per device.

```python
import jax
import jax.numpy as jnp
from jax import lax

D = 768
HEADS = 12
HEAD_DIM = 32
WIN_Z = 2
WIN_LAT = 6
WIN_LON = 12
LEVELS = 4
WIN_TOK = 144
BIAS_POS = 3312
LAT = 24
LON = 96
LAT_WIN = 4
Z_WIN = 2


def index_helper(key):
    return jax.random.randint(jax.random.fold_in(key, 11), (WIN_TOK, WIN_TOK), 0, BIAS_POS, dtype=jnp.int32)


def draw_index_table(key, part):
    return index_helper(key)


def draw_bias_table(key, part):
    inner_key = jax.random.fold_in(key, 23)
    full_shape = (LAT_WIN, Z_WIN, HEADS, BIAS_POS)
    entries = jnp.clip(jax.random.normal(inner_key, full_shape, jnp.float32), -3.5, 3.5)
    return entries.astype(jnp.bfloat16)


def draw_state_tokens(key, part):
    subkeys = jax.random.split(jax.random.fold_in(key, 5), 3)
    full_shape = (LEVELS, LAT, LON, D)
    normal_part = jnp.clip(jax.random.normal(subkeys[0], full_shape, jnp.float32), -3.5, 3.5)
    row_scale = jnp.exp(jax.random.uniform(subkeys[1], (LEVELS, LAT, LON, 1), jnp.float32, jnp.log(0.3), jnp.log(3.0)))
    column_scale = jnp.exp(jax.random.uniform(subkeys[2], (D,), jnp.float32, jnp.log(0.3), jnp.log(3.0)))
    drawn_values = normal_part * row_scale * column_scale
    return drawn_values.astype(jnp.bfloat16)


def draw_pad_mask(key, part):
    subkeys = jax.random.split(jax.random.fold_in(key, 31), 2)
    other_end = jax.random.randint(subkeys[0], (), 0, 3, dtype=jnp.int32)
    chosen = jax.random.randint(subkeys[1], (), 0, 2, dtype=jnp.int32)
    north_rows = jnp.where(chosen == 0, 2, other_end)
    south_rows = jnp.where(chosen == 0, other_end, 2)
    positions = jnp.arange(LAT, dtype=jnp.int32)
    row_mask = (positions >= north_rows) & (positions < LAT - south_rows)
    return row_mask.astype(jnp.int32)


def place_ends(result, rng, smallest, high):
    spot = [jax.random.randint(jax.random.fold_in(rng, axis), (), 0, length) for axis, length in enumerate(result.shape)]
    main_axis = result.shape.index(max(result.shape))
    neighbour = spot[:main_axis] + [(spot[main_axis] + 1) % result.shape[main_axis]] + spot[main_axis + 1:]
    return result.at[tuple(spot)].set(smallest).at[tuple(neighbour)].set(high)


def scatter_about(own_key, extent, width, bound, held_as=jnp.bfloat16):
    return jnp.clip(width * jax.random.normal(own_key, extent, jnp.float32), -bound, bound).astype(held_as)


def setup_inputs(seed: int = 0, part: int = 0) -> dict:
    seeds = jax.random.split(jax.random.key(seed), 12)
    part_splits = jax.random.split(jax.random.fold_in(seeds[11], part), 12)
    state_tokens = draw_state_tokens(jax.random.fold_in(jax.random.fold_in(seeds[11], part), 71), part)
    land_mask = place_ends((jax.random.randint(seeds[1], (LAT, LON), 0, 3) < 1).astype(jnp.int32), jax.random.fold_in(seeds[1], 1), 0, 1)
    pad_mask = draw_pad_mask(jax.random.fold_in(seeds[11], 71), part)
    land_embed = scatter_about(seeds[3], (2, D), 0.5, 3.0, jnp.float32)
    w_qkv = scatter_about(seeds[4], (D, 3 * HEADS * HEAD_DIM), D ** -0.5, 0.21875)
    w_proj = scatter_about(seeds[5], (HEADS * HEAD_DIM, D), (HEADS * HEAD_DIM) ** -0.5, 0.3125)
    proj_bias = scatter_about(seeds[6], (D,), 1.0, 4.0, jnp.float32)
    norm_gain = jnp.clip(1.0 + 0.1 * jax.random.normal(seeds[7], (D,), jnp.float32), 0.5, 1.5)
    norm_shift = scatter_about(seeds[8], (D,), 0.3, 1.5, jnp.float32)
    bias_table = draw_bias_table(jax.random.fold_in(seeds[11], 71), part)
    index_table = draw_index_table(jax.random.fold_in(seeds[11], 71), part)
    return dict(state_tokens=state_tokens, land_mask=land_mask, pad_mask=pad_mask, land_embed=land_embed, w_qkv=w_qkv, w_proj=w_proj, proj_bias=proj_bias, norm_gain=norm_gain, norm_shift=norm_shift, bias_table=bias_table, index_table=index_table)


norm_epsilon = 1e-05

def region_of(position, length, window):
    half_window = window // 2
    return jnp.where(position < length - window, 0, jnp.where(position < length - half_window, 1, 2)).astype(jnp.int32)

def window_rules(levels, lat_start, lat_rows, lat_total, pad_mask):
    tokens = jnp.arange(WIN_TOK, dtype=jnp.int32)
    level_offset = tokens // (WIN_LAT * WIN_LON)
    row_offset = tokens // WIN_LON % WIN_LAT
    level_index = jnp.arange(levels // WIN_Z, dtype=jnp.int32)[:, None] * WIN_Z + level_offset[None, :]
    row_index = lat_start + jnp.arange(lat_rows // WIN_LAT, dtype=jnp.int32)[:, None] * WIN_LAT + row_offset[None, :]
    region = region_of(level_index, levels, WIN_Z)[:, None, :] * 3 + region_of(row_index, lat_total, WIN_LAT)[None, :, :]
    source_row = (row_index + WIN_LAT // 2) % lat_total
    lookup = (source_row[:, :, None] == jnp.arange(lat_total, dtype=jnp.int32)[None, None, :]).astype(jnp.int32)
    usable = lax.optimization_barrier(jnp.sum(lookup * pad_mask[None, None, :], axis=-1)) == 1
    return (region[:, :, :, None] == region[:, :, None, :]) & usable[None, :, None, :]

def earth_bias(bias_table, index_table):
    gathered = jnp.take(bias_table, index_table, axis=3).astype(jnp.float32)
    return jnp.transpose(gathered, (1, 0, 2, 3, 4))

def to_windows(layout):
    levels, lat_rows, lon_columns, channels = layout.shape
    shaped = layout.reshape(levels // WIN_Z, WIN_Z, lat_rows // WIN_LAT, WIN_LAT, lon_columns // WIN_LON, WIN_LON, channels)
    shaped = shaped.transpose(0, 2, 4, 1, 3, 5, 6)
    return shaped.reshape(levels // WIN_Z, lat_rows // WIN_LAT, lon_columns // WIN_LON, WIN_TOK, channels)

def from_windows(window_tiles):
    z_windows, lat_windows, lon_windows, tokens, channels = window_tiles.shape
    shaped = window_tiles.reshape(z_windows, lat_windows, lon_windows, WIN_Z, WIN_LAT, WIN_LON, channels)
    shaped = shaped.transpose(0, 3, 1, 4, 2, 5, 6)
    return shaped.reshape(z_windows * WIN_Z, lat_windows * WIN_LAT, lon_windows * WIN_LON, channels)

def attend(projections, bias_full, allowed):
    pieces = projections.astype(jnp.float32).reshape(projections.shape[:-1] + (3, HEADS, HEAD_DIM))
    queries = pieces[..., 0, :, :]
    key_rows = pieces[..., 1, :, :]
    value_rows = pieces[..., 2, :, :]
    scores = jnp.einsum('abthd,abuhd->abhtu', queries, key_rows) / jnp.sqrt(jnp.float32(HEAD_DIM)) + bias_full
    scores = jnp.where(allowed[:, :, None], scores, -jnp.inf)
    largest = lax.optimization_barrier(jnp.max(scores, axis=-1, keepdims=True))
    powers = jnp.exp(scores - largest)
    weights = (powers / lax.optimization_barrier(jnp.sum(powers, axis=-1, keepdims=True))).astype(jnp.bfloat16)
    attended = jnp.einsum('abhtu,abuhd->abthd', weights.astype(jnp.float32), value_rows).astype(jnp.bfloat16)
    return attended.reshape(attended.shape[:3] + (HEADS * HEAD_DIM,))

def finish(attended, w_proj, proj_bias, norm_gain, norm_shift):
    projected = jnp.dot(attended, w_proj, preferred_element_type=jnp.float32) + proj_bias
    average = lax.optimization_barrier(jnp.mean(projected, axis=-1, keepdims=True))
    centered = projected - average
    spread = lax.optimization_barrier(jnp.mean(centered * centered, axis=-1, keepdims=True))
    return centered * lax.rsqrt(spread + norm_epsilon) * norm_gain + norm_shift

def reference(state_tokens, land_mask, pad_mask, land_embed, w_qkv, w_proj, proj_bias, norm_gain, norm_shift, bias_table, index_table):
    embedded = jnp.where(land_mask[:, :, None] == 1, land_embed[1], land_embed[0])
    hidden = (state_tokens.astype(jnp.float32) + embedded[None]).astype(jnp.bfloat16)
    shifted = jnp.roll(hidden, (-(WIN_Z // 2), -(WIN_LAT // 2), -(WIN_LON // 2)), axis=(0, 1, 2))
    windows = jnp.moveaxis(to_windows(shifted), 2, 0)
    bias_full = earth_bias(bias_table, index_table)
    allowed = window_rules(LEVELS, 0, LAT, LAT, pad_mask)

    def one_column(column_block):
        projections = jnp.dot(column_block, w_qkv, preferred_element_type=jnp.float32).astype(jnp.bfloat16)
        return finish(attend(projections, bias_full, allowed), w_proj, proj_bias, norm_gain, norm_shift)
    normed = lax.map(one_column, windows)
    layout = from_windows(jnp.moveaxis(normed, 0, 2))
    restored = jnp.roll(layout, (WIN_Z // 2, WIN_LAT // 2, WIN_LON // 2), axis=(0, 1, 2))
    return (hidden.astype(jnp.float32) + restored).astype(jnp.bfloat16)
```

```python
import jax
import jax.numpy as jnp
import numpy as np
from jax import lax
from jax.experimental import pallas as pl
from jax.experimental.pallas import tpu as pltpu
from jax.sharding import PartitionSpec as P

HEADS = 12
HEAD_DIM = 32
WIN_Z = 2
WIN_LAT = 6
WIN_LON = 12
WIN_TOK = 144
HALF_LAT = WIN_LAT // 2
HALF_LON = WIN_LON // 2
GROUP = WIN_Z * HALF_LAT * HALF_LON
SLOT = 48
LOW = 256
SHUT = -1e30
WIDTH = HEADS * HEAD_DIM

norm_epsilon = 1e-05


def from_behind(shard, axis, by):
    size = lax.axis_size(axis)
    return lax.ppermute(shard, axis, [(i, (i + by) % size) for i in range(size)])


def group_tokens(a, b):
    dz, di, dj = np.meshgrid(
        np.arange(WIN_Z), np.arange(HALF_LAT), np.arange(HALF_LON), indexing="ij"
    )
    return ((dz * WIN_LAT + a * HALF_LAT + di) * WIN_LON + b * HALF_LON + dj).reshape(-1)


def window_orders():
    groups = [group_tokens(a, b) for a in range(2) for b in range(2)]
    queries = np.concatenate(groups)
    keys = np.concatenate([g[:32] for g in groups] + [g[32:] for g in groups])
    return queries, keys


def token_orders(levels, lat_rows, lon_columns):
    quarters = lat_rows // HALF_LAT
    z_windows = levels // WIN_Z
    rows = 2 * quarters * z_windows * SLOT
    placed = np.full((rows,), -1, np.int32)
    plain = np.full((rows,), -1, np.int32)
    row = 0
    for lon_half in range(2):
        for quarter in range(quarters):
            for zw in range(z_windows):
                a, b = 1 - quarter % 2, 1 - lon_half
                t = 0
                for dz in range(WIN_Z):
                    for di in range(HALF_LAT):
                        for dj in range(HALF_LON):
                            z = (zw * WIN_Z + dz + WIN_Z // 2) % levels
                            i = quarter * HALF_LAT + di
                            j = lon_half * HALF_LON + dj
                            natural = (z * lat_rows + i) * 16 + j
                            place = t if t < 32 else t + 4 * (2 * a + b)
                            placed[row + place] = natural
                            plain[row + t] = natural
                            t += 1
                row += SLOT
    return placed, plain


def bias_kernel(meta_ref, table_ref, out_ref):
    highs = table_ref.shape[1] // 48
    half_row = lax.broadcasted_iota(jnp.int32, (8, LOW), 0) < 4
    low_iota = lax.broadcasted_iota(jnp.int32, (LOW, LOW), 0)

    def look_up(a, tile):
        meta = meta_ref[tile]
        hot = jnp.where(low_iota == meta[0:1], 1.0, 0.0).astype(jnp.bfloat16)
        found = jnp.dot(table_ref[a], hot, preferred_element_type=jnp.float32)
        high = jnp.broadcast_to(meta[1:2], (48, LOW))
        total = found[0:48]
        for k in range(1, highs):
            total = jnp.where(high == k, found[k * 48 : (k + 1) * 48], total)
        pieces = []
        for s in range(2):
            first = jnp.broadcast_to(meta[2 + 2 * s : 3 + 2 * s], (8, LOW))
            second = jnp.broadcast_to(meta[3 + 2 * s : 4 + 2 * s], (8, LOW))
            for kind, allowed in enumerate((first, second, jnp.where(half_row, first, second))):
                part = total[(s * 3 + kind) * 8 : (s * 3 + kind) * 8 + 8]
                pieces.append(jnp.where(allowed == 1, part, SHUT))
        return pieces

    for a in range(2):

        def pair(p, carry, a=a):
            pieces = look_up(a, a * 36 + p)
            for s in range(2):
                for kind in range(3):
                    part = pieces[s * 3 + kind]
                    out_ref[a, s, kind, 2 * p, :, 0:128] = part[:, 0:128]
                    out_ref[a, s, kind, 2 * p + 1, :, 0:128] = part[:, 128:256]
            return carry

        lax.fori_loop(0, 36, pair, 0)
        for tile in range(5):
            pieces = look_up(a, 72 + a * 5 + tile)
            for j in range(16):
                q = tile * 16 + j
                if q < 72:
                    for s in range(2):
                        for kind in range(3):
                            out_ref[a, s, kind, q, :, 128:144] = pieces[s * 3 + kind][
                                :, 16 * j : 16 * j + 16
                            ]


def attend_kernel(
    bias_ref,
    q_ref,
    own_ref,
    left_ref,
    right_ref,
    up_ref,
    down_ref,
    hidden_ref,
    restore_ref,
    w_ref,
    vectors_ref,
    out_ref,
    keys_ref,
    attended_ref,
):
    step = pl.program_id(0)

    @pl.when(step == 0)
    def _():
        def column(c, quarter, zw):
            if quarter < 0:
                return up_ref.at[c, zw]
            if quarter > 3:
                return down_ref.at[c, zw]
            if c == 0:
                return left_ref.at[quarter, zw]
            if c == 3:
                return right_ref.at[quarter, zw]
            return own_ref.at[c - 1, quarter, zw]

        for lat in range(3):
            for lon in range(2):
                for zw in range(2):
                    rest = None
                    for a in range(2):
                        for b in range(2):
                            ref = column(2 * lon + b, 2 * lat - 1 + a, zw)
                            n = 32 * (2 * a + b)
                            keys_ref[2 * lat + lon, zw, n : n + 32, :] = ref[0:32, :]
                            tail = ref[32:48, :]
                            rest = tail if rest is None else rest + tail
                    keys_ref[2 * lat + lon, zw, 128:144, :] = rest

    quarter, lon = step // 2, step % 2
    window = 2 * ((quarter + 1) // 2) + lon
    head_mask = jnp.where(
        lax.broadcasted_iota(jnp.int32, (8, 256), 1) // HEAD_DIM
        == lax.broadcasted_iota(jnp.int32, (8, 256), 0),
        1.0,
        0.0,
    )
    gather_rows = jnp.where(
        lax.broadcasted_iota(jnp.int32, (SLOT, 8 * GROUP), 1) // 8
        == lax.broadcasted_iota(jnp.int32, (SLOT, 8 * GROUP), 0),
        1.0,
        0.0,
    ).astype(jnp.bfloat16)
    queries = []
    for zw in range(2):
        q = q_ref[lon, quarter, zw].astype(jnp.float32)
        tail = (q[32:36] + q[36:40]) + (q[40:44] + q[44:48])
        queries.append(jnp.concatenate([q[0:32], tail], axis=0))
    results = []
    for kind in range(3):
        if kind < 2:
            q = queries[kind][:, 0:256]
            key = keys_ref[window, kind, :, 0:256]
            value = keys_ref[window, kind, :, WIDTH : WIDTH + 256]
        else:
            q = jnp.concatenate([queries[0][:, 256:384], queries[1][:, 256:384]], axis=1)
            key = jnp.concatenate(
                [keys_ref[window, 0, :, 256:384], keys_ref[window, 1, :, 256:384]], axis=1
            )
            value = jnp.concatenate(
                [keys_ref[window, 0, :, 640:768], keys_ref[window, 1, :, 640:768]], axis=1
            )
        spread = (q[:, None, :] * head_mask[None]).reshape(8 * GROUP, 256).astype(jnp.bfloat16)
        scores = lax.dot_general(
            spread, key, (((1,), (1,)), ((), ())), preferred_element_type=jnp.float32
        )
        bias = bias_ref[0, 0, kind].reshape(8 * GROUP, 256)[:, 0:WIN_TOK]
        scores = scores * (HEAD_DIM**-0.5) + bias
        powers = jnp.exp(scores - jnp.max(scores, axis=-1, keepdims=True))
        weights = (powers / jnp.sum(powers, axis=-1, keepdims=True)).astype(jnp.bfloat16)
        mixed = jnp.dot(weights, value, preferred_element_type=jnp.float32)
        mixed = (mixed.reshape(GROUP, 8, 256) * head_mask[None]).reshape(8 * GROUP, 256)
        results.append(
            jnp.dot(
                gather_rows, mixed.astype(jnp.bfloat16), preferred_element_type=jnp.float32
            ).astype(jnp.bfloat16)
        )
    for zw in range(2):
        row = ((lon * 4 + quarter) * 2 + zw) * SLOT
        row = pl.multiple_of(row, SLOT)
        attended_ref[pl.ds(row, SLOT), 0:256] = results[zw]
        attended_ref[pl.ds(row, SLOT), 256:384] = results[2][:, zw * 128 : zw * 128 + 128]

    @pl.when(step == pl.num_programs(0) - 1)
    def _():
        chunk = 192
        for n in range(0, hidden_ref.shape[0], chunk):
            natural = jnp.dot(
                restore_ref[n : n + chunk, :],
                attended_ref[...],
                preferred_element_type=jnp.float32,
            ).astype(jnp.bfloat16)
            projected = (
                jnp.dot(natural, w_ref[...], preferred_element_type=jnp.float32)
                + vectors_ref[0:1, :]
            )
            centered = projected - jnp.mean(projected, axis=-1, keepdims=True)
            spread = jnp.mean(centered * centered, axis=-1, keepdims=True)
            normed = (
                centered * lax.rsqrt(spread + norm_epsilon) * vectors_ref[1:2, :]
                + vectors_ref[2:3, :]
            )
            result = (hidden_ref[n : n + chunk, :].astype(jnp.float32) + normed).astype(
                jnp.bfloat16
            )
            result = result.reshape(chunk // 16, 16, result.shape[-1])
            out_ref[n // 16 : (n + chunk) // 16] = result[:, : out_ref.shape[1], :]


def allowed_pairs(lat_index, lat_total, pad_mask):
    queries, keys = window_orders()
    windows = lat_total // WIN_LAT
    q_level, q_half = queries // 72, queries // 12 % 6 // 3
    k_level, k_row = keys // 72, keys // 12 % 6
    base = 2 * lat_index
    edge = jnp.where(jnp.asarray(q_half == 1), base - 1 + windows, base + 1) % windows
    rows = []
    for window in (edge, jnp.zeros_like(edge) + base):
        source = (window[:, None] * WIN_LAT + jnp.asarray(k_row)[None, :] + HALF_LAT) % lat_total
        usable = jnp.zeros(source.shape, jnp.int32)
        for n in range(pad_mask.shape[0]):
            usable = jnp.where(source == n, pad_mask[n], usable)
        same_half = jnp.asarray(q_half[:, None] == (k_row // 3)[None, :])
        same_row = (window[:, None] != windows - 1) | same_half
        for zw in range(2):
            same_level = jnp.asarray((zw == 0) | (q_level[:, None] == k_level[None, :]))
            rows.append(((usable == 1) & same_row & same_level).astype(jnp.int32))
    return rows


def as_tiles(rows):
    main = rows[:, :128].reshape(72, 256)
    rest = jnp.pad(rows[:, 128:].reshape(2, 72, 16), ((0, 0), (0, 8), (0, 0))).reshape(10, 256)
    return jnp.concatenate([main, rest], axis=0)


def bias_inputs(bias_table, index_table, pad_mask, lat_index, lat_total):
    queries, keys = window_orders()
    to_q = jnp.asarray(np.eye(WIN_TOK)[queries], jnp.bfloat16)
    to_k = jnp.asarray(np.eye(WIN_TOK)[keys].T, jnp.bfloat16)

    def reorder(values):
        picked = jnp.dot(to_q, values.astype(jnp.bfloat16), preferred_element_type=jnp.float32)
        picked = jnp.dot(picked.astype(jnp.bfloat16), to_k, preferred_element_type=jnp.float32)
        return picked.astype(jnp.int32)

    rows = [reorder(index_table % LOW), reorder(index_table // LOW)]
    rows += allowed_pairs(lat_index, lat_total, pad_mask)
    meta = jnp.stack([as_tiles(r) for r in rows], axis=1)
    before = from_behind(bias_table[-1], "lat", 1)
    positions = bias_table.shape[-1]
    highs = -(-positions // LOW)

    def kinds(table):
        table = jnp.pad(table, ((0, 0), (0, 0), (0, highs * LOW - positions)))
        last = jnp.concatenate([table[0, 8:], table[1, 8:]], axis=0)
        return jnp.stack([table[0, :8], table[1, :8], last])

    first, second, third = kinds(before), kinds(bias_table[0]), kinds(bias_table[1])
    tables = jnp.stack([jnp.stack([third, second]), jnp.stack([first, second])])
    tables = tables.reshape(2, 48, highs, LOW).transpose(0, 2, 1, 3).reshape(2, highs * 48, LOW)
    return meta, tables


def on_device(
    state_tokens,
    land_mask,
    pad_mask,
    land_embed,
    w_qkv,
    w_proj,
    proj_bias,
    norm_gain,
    norm_shift,
    bias_table,
    index_table,
):
    levels, lat_rows, lon_columns, features = state_tokens.shape
    assert (levels, lat_rows, lon_columns) == (2 * WIN_Z, 2 * WIN_LAT, WIN_LON)
    lat_total = lat_rows * lax.axis_size("lat")
    embedded = jnp.where(land_mask[:, :, None] == 1, land_embed[1], land_embed[0])
    hidden = (state_tokens.astype(jnp.float32) + embedded[None]).astype(jnp.bfloat16)
    hidden = jnp.pad(hidden, ((0, 0), (0, 0), (0, 16 - lon_columns), (0, 0)))
    hidden = hidden.reshape(levels * lat_rows * 16, features)
    rows = hidden.shape[0]
    placed, plain = token_orders(levels, lat_rows, lon_columns)
    natural = jnp.arange(rows, dtype=jnp.int32)
    to_groups = (jnp.asarray(placed)[:, None] == natural[None, :]).astype(jnp.bfloat16)
    restore = (natural[:, None] == jnp.asarray(plain)[None, :]).astype(jnp.bfloat16)
    grouped = jnp.dot(to_groups, hidden, preferred_element_type=jnp.float32).astype(jnp.bfloat16)
    shape = (2, 4, 2, SLOT)
    kv = jnp.dot(grouped, w_qkv[:, WIDTH:], preferred_element_type=jnp.float32)
    kv = kv.astype(jnp.bfloat16).reshape(shape + (2 * WIDTH,))
    right = from_behind(kv[0], "lon", -1)
    left = from_behind(kv[1], "lon", 1)
    up = from_behind(jnp.stack([left[3], kv[0, 3], kv[1, 3], right[3]]), "lat", 1)
    down = from_behind(jnp.stack([left[0], kv[0, 0], kv[1, 0], right[0]]), "lat", -1)
    q = jnp.dot(grouped, w_qkv[:, :WIDTH], preferred_element_type=jnp.float32)
    q = q.astype(jnp.bfloat16).reshape(shape + (WIDTH,))
    meta, tables = bias_inputs(bias_table, index_table, pad_mask, lax.axis_index("lat"), lat_total)
    bias = pl.pallas_call(
        bias_kernel,
        out_shape=jax.ShapeDtypeStruct((2, 2, 3, 72, 8, 256), jnp.float32),
        in_specs=[pl.BlockSpec(memory_space=pltpu.VMEM)] * 2,
        out_specs=pl.BlockSpec(memory_space=pltpu.VMEM),
        compiler_params=pltpu.CompilerParams(vmem_limit_bytes=24 << 20),
        cost_estimate=pl.CostEstimate(
            flops=2 * 82 * 624 * 256 * 256, bytes_accessed=8 << 20, transcendentals=0
        ),
        name="bias",
    )(meta, tables)
    vectors = jnp.stack([proj_bias, norm_gain, norm_shift])
    whole = pl.BlockSpec(memory_space=pltpu.VMEM)

    def bias_block(i):
        quarter, lon = i // 2, i % 2
        return (1 - quarter % 2, (quarter + 1) // 2 % 2, 0, 1 - lon, 0, 0)

    out = pl.pallas_call(
        attend_kernel,
        grid=(8,),
        out_shape=jax.ShapeDtypeStruct((levels * lat_rows, lon_columns, features), jnp.bfloat16),
        in_specs=[pl.BlockSpec((1, 1, 3, GROUP, 8, 256), bias_block)] + [whole] * 10,
        out_specs=whole,
        scratch_shapes=[
            pltpu.VMEM((6, 2, WIN_TOK, 2 * WIDTH), jnp.bfloat16),
            pltpu.VMEM((rows, WIDTH), jnp.bfloat16),
        ],
        compiler_params=pltpu.CompilerParams(
            vmem_limit_bytes=40 << 20, dimension_semantics=("arbitrary",)
        ),
        name="attend",
    )(bias, q, kv, left, right, up, down, hidden, restore, w_proj, vectors)
    return out.reshape(state_tokens.shape)


def solution(mesh):
    in_specs = (
        P("member", "lat", "lon", None),
        P("lat", "lon"),
        P(),
        P(),
        P(),
        P(),
        P(),
        P(),
        P(),
        P("lat", None, None, None),
        P(),
    )
    out_specs = P("member", "lat", "lon", None)
    return jax.shard_map(
        on_device, mesh=mesh, in_specs=in_specs, out_specs=out_specs, check_vma=False
    )
```

```python
import jax
import jax.numpy as jnp
import numpy as np
from jax import lax
from jax.experimental import pallas as pl
from jax.experimental.pallas import tpu as pltpu
from jax.sharding import PartitionSpec as P

HEADS = 12
HEAD_DIM = 32
WIN_Z = 2
WIN_LAT = 6
WIN_LON = 12
WIN_TOK = 144
HALF_LAT = WIN_LAT // 2
HALF_LON = WIN_LON // 2
GROUP = WIN_Z * HALF_LAT * HALF_LON
SLOT = 48
LOW = 256
SHUT = -1e30
WIDTH = HEADS * HEAD_DIM

norm_epsilon = 1e-05


def from_behind(shard, axis, by):
    size = lax.axis_size(axis)
    return lax.ppermute(shard, axis, [(i, (i + by) % size) for i in range(size)])


def group_tokens(a, b):
    dz, di, dj = np.meshgrid(
        np.arange(WIN_Z), np.arange(HALF_LAT), np.arange(HALF_LON), indexing="ij"
    )
    return ((dz * WIN_LAT + a * HALF_LAT + di) * WIN_LON + b * HALF_LON + dj).reshape(-1)


def window_orders():
    groups = [group_tokens(a, b) for a in range(2) for b in range(2)]
    queries = np.concatenate(groups)
    keys = np.concatenate([g[:32] for g in groups] + [g[32:] for g in groups])
    return queries, keys


def token_orders(levels, lat_rows, lon_columns):
    quarters = lat_rows // HALF_LAT
    z_windows = levels // WIN_Z
    rows = 2 * quarters * z_windows * SLOT
    placed = np.full((rows,), -1, np.int32)
    plain = np.full((rows,), -1, np.int32)
    row = 0
    for lon_half in range(2):
        for quarter in range(quarters):
            for zw in range(z_windows):
                a, b = 1 - quarter % 2, 1 - lon_half
                t = 0
                for dz in range(WIN_Z):
                    for di in range(HALF_LAT):
                        for dj in range(HALF_LON):
                            z = (zw * WIN_Z + dz + WIN_Z // 2) % levels
                            i = quarter * HALF_LAT + di
                            j = lon_half * HALF_LON + dj
                            natural = (z * lat_rows + i) * 16 + j
                            place = t if t < 32 else t + 4 * (2 * a + b)
                            placed[row + place] = natural
                            plain[row + t] = natural
                            t += 1
                row += SLOT
    return placed, plain


def bias_kernel(
    index_ref,
    before_ref,
    own_ref,
    pad_ref,
    lat_ref,
    to_q_ref,
    to_k_ref,
    to_q_rest_ref,
    to_k_rest_ref,
    geometry_ref,
    out_ref,
    low_ref,
    high_ref,
    table_ref,
):
    positions = own_ref.shape[-1]
    highs = table_ref.shape[1] // 48
    half_row = lax.broadcasted_iota(jnp.int32, (8, LOW), 0) < 4
    low_iota = lax.broadcasted_iota(jnp.int32, (LOW, LOW), 0)

    def dot(x, y):
        return jnp.dot(x, y, preferred_element_type=jnp.float32)

    index = index_ref[...]
    rest_lane = lax.broadcasted_iota(jnp.int32, (160, LOW), 1) // 16
    rest_row = lax.broadcasted_iota(jnp.int32, (160, LOW), 0) % 16
    gather = jnp.where(
        lax.broadcasted_iota(jnp.int32, (16, 160), 1) // 16
        == lax.broadcasted_iota(jnp.int32, (16, 160), 0),
        1.0,
        0.0,
    ).astype(jnp.bfloat16)
    for values, ref in ((index % LOW, low_ref), (index // LOW, high_ref)):
        values = values.astype(jnp.float32).astype(jnp.bfloat16)
        main = dot(dot(to_q_ref[...], values).astype(jnp.bfloat16), to_k_ref[...])
        ref[0:WIN_TOK, :] = main.astype(jnp.int32)
        rest = dot(dot(to_q_rest_ref[...], values).astype(jnp.bfloat16), to_k_rest_ref[...])
        rest = jnp.where(rest_lane == rest_row, rest, 0.0).astype(jnp.bfloat16)
        rest = dot(gather, rest).astype(jnp.int32)
        ref[WIN_TOK : WIN_TOK + 16, :] = rest[:, 0:128]
        ref[WIN_TOK + 16 : WIN_TOK + 32, :] = rest[:, 128:256]

    for k in range(highs):
        end = min(positions, (k + 1) * LOW)
        sides = []
        for window in range(3):
            parts = []
            for zw in range(WIN_Z):
                ref = before_ref if window == 0 else own_ref.at[window - 1]
                part = ref[zw, :, k * LOW : end].astype(jnp.float32)
                if end < (k + 1) * LOW:
                    fill = jnp.zeros((part.shape[0], (k + 1) * LOW - end), jnp.float32)
                    part = jnp.concatenate([part, fill], axis=1)
                parts.append(part)
            sides.append([parts[0][:8], parts[1][:8], parts[0][8:], parts[1][8:]])
        for a, edge in ((0, 2), (1, 0)):
            block = jnp.concatenate(sides[edge] + sides[1], axis=0)
            table_ref[a, k * 48 : (k + 1) * 48, :] = block.astype(jnp.bfloat16)

    lat_total = pad_ref.shape[0]
    windows = lat_total // WIN_LAT
    base = 2 * lat_ref[0]

    def look_up(a, tile, low, high):
        hot = jnp.where(low_iota == low, 1.0, 0.0).astype(jnp.bfloat16)
        found = dot(table_ref[a], hot)
        high = jnp.broadcast_to(high, (48, LOW))
        total = found[0:48]
        for k in range(1, highs):
            total = jnp.where(high == k, found[k * 48 : (k + 1) * 48], total)
        geometry = geometry_ref[tile]
        key_row, same_half, same_level = geometry[0:1], geometry[1:2], geometry[2:3]
        pieces = []
        for s in range(2):
            window = base
            if s == 0:
                window = lax.rem(base - 1 + windows if a == 1 else base + 1, windows)
            usable = jnp.zeros((1, LOW), jnp.int32)
            for n in range(WIN_LAT):
                source = lax.rem(window * WIN_LAT + n + HALF_LAT, lat_total)
                usable = jnp.where(key_row == n, pad_ref[source], usable)
            inner = (window != windows - 1).astype(jnp.int32)
            usable = jnp.where(usable == 1, jnp.maximum(same_half, inner), 0)
            first = jnp.broadcast_to(usable, (8, LOW))
            second = jnp.broadcast_to(usable * same_level, (8, LOW))
            for kind, allowed in enumerate((first, second, jnp.where(half_row, first, second))):
                part = total[(s * 3 + kind) * 8 : (s * 3 + kind) * 8 + 8]
                pieces.append(jnp.where(allowed == 1, part, SHUT))
        return pieces

    def both(x, y):
        return jnp.concatenate([x, y], axis=0).astype(jnp.bfloat16)

    for a in range(2):

        def pair(p, carry, a=a):
            tile = a * 36 + p

            def two(ref):
                return jnp.concatenate(
                    [ref[pl.ds(2 * tile, 1), :], ref[pl.ds(2 * tile + 1, 1), :]], axis=1
                )

            pieces = look_up(a, tile, two(low_ref), two(high_ref))
            for s in range(2):
                for kind in range(3):
                    part = pieces[s * 3 + kind]
                    out_ref[a, s, kind, p, :, 0:128] = both(part[:, 0:128], part[:, 128:256])
            return carry

        lax.fori_loop(0, 36, pair, 0)
        for tile in range(5):
            row = WIN_TOK + a * 5 + tile

            def wide(ref, row=row):
                return jnp.concatenate([ref[row : row + 1, :], ref[row + 16 : row + 17, :]], axis=1)

            pieces = look_up(a, 72 + a * 5 + tile, wide(low_ref), wide(high_ref))
            for j in range(0, 16, 2):
                q = tile * 16 + j
                if q < 72:
                    for s in range(2):
                        for kind in range(3):
                            part = pieces[s * 3 + kind]
                            out_ref[a, s, kind, q // 2, :, 128:144] = both(
                                part[:, 16 * j : 16 * j + 16], part[:, 16 * j + 16 : 16 * j + 32]
                            )


def attend_kernel(
    bias_ref,
    own_ref,
    left_ref,
    right_ref,
    up_ref,
    down_ref,
    hidden_ref,
    restore_ref,
    w_ref,
    offset_ref,
    gain_ref,
    shift_ref,
    out_ref,
    keys_ref,
    attended_ref,
):
    step = pl.program_id(0)

    @pl.when(step == 0)
    def _():
        def column(c, quarter, zw):
            if quarter < 0:
                return up_ref.at[c, zw]
            if quarter > 3:
                return down_ref.at[c, zw]
            if c == 0:
                return left_ref.at[quarter, zw]
            if c == 3:
                return right_ref.at[quarter, zw]
            return own_ref.at[c - 1, quarter, zw, :, WIDTH : 3 * WIDTH]

        for lat in range(3):
            for lon in range(2):
                for zw in range(2):
                    rest = None
                    for a in range(2):
                        for b in range(2):
                            ref = column(2 * lon + b, 2 * lat - 1 + a, zw)
                            n = 32 * (2 * a + b)
                            keys_ref[2 * lat + lon, zw, n : n + 32, :] = ref[0:32, :]
                            tail = ref[32:48, :]
                            rest = tail if rest is None else rest + tail
                    keys_ref[2 * lat + lon, zw, 128:144, :] = rest

    quarter, lon = step // 2, step % 2
    window = 2 * ((quarter + 1) // 2) + lon
    head_mask = jnp.where(
        lax.broadcasted_iota(jnp.int32, (8, 256), 1) // HEAD_DIM
        == lax.broadcasted_iota(jnp.int32, (8, 256), 0),
        1.0,
        0.0,
    )
    gather_rows = jnp.where(
        lax.broadcasted_iota(jnp.int32, (SLOT, 8 * GROUP), 1) // 8
        == lax.broadcasted_iota(jnp.int32, (SLOT, 8 * GROUP), 0),
        1.0,
        0.0,
    ).astype(jnp.bfloat16)
    queries = []
    for zw in range(2):
        q = own_ref[lon, quarter, zw, :, 0:WIDTH].astype(jnp.float32)
        tail = (q[32:36] + q[36:40]) + (q[40:44] + q[44:48])
        queries.append(jnp.concatenate([q[0:32], tail], axis=0))
    results = []
    for kind in range(3):
        if kind < 2:
            q = queries[kind][:, 0:256]
            key = keys_ref[window, kind, :, 0:256]
            value = keys_ref[window, kind, :, WIDTH : WIDTH + 256]
        else:
            q = jnp.concatenate([queries[0][:, 256:384], queries[1][:, 256:384]], axis=1)
            key = jnp.concatenate(
                [keys_ref[window, 0, :, 256:384], keys_ref[window, 1, :, 256:384]], axis=1
            )
            value = jnp.concatenate(
                [keys_ref[window, 0, :, 640:768], keys_ref[window, 1, :, 640:768]], axis=1
            )
        spread = (q[:, None, :] * head_mask[None]).reshape(8 * GROUP, 256).astype(jnp.bfloat16)
        scores = lax.dot_general(
            spread, key, (((1,), (1,)), ((), ())), preferred_element_type=jnp.float32
        )
        bias = bias_ref[0, 0, kind].reshape(8 * GROUP, 256)[:, 0:WIN_TOK]
        bias = bias.astype(jnp.float32)
        scores = scores * (HEAD_DIM**-0.5) + bias
        powers = jnp.exp(scores - jnp.max(scores, axis=-1, keepdims=True))
        weights = (powers / jnp.sum(powers, axis=-1, keepdims=True)).astype(jnp.bfloat16)
        mixed = jnp.dot(weights, value, preferred_element_type=jnp.float32)
        mixed = (mixed.reshape(GROUP, 8, 256) * head_mask[None]).reshape(8 * GROUP, 256)
        results.append(
            jnp.dot(
                gather_rows, mixed.astype(jnp.bfloat16), preferred_element_type=jnp.float32
            ).astype(jnp.bfloat16)
        )
    for zw in range(2):
        row = ((lon * 4 + quarter) * 2 + zw) * SLOT
        row = pl.multiple_of(row, SLOT)
        attended_ref[pl.ds(row, SLOT), 0:256] = results[zw]
        attended_ref[pl.ds(row, SLOT), 256:384] = results[2][:, zw * 128 : zw * 128 + 128]

    @pl.when(step == pl.num_programs(0) - 1)
    def _():
        chunk = 192
        for n in range(0, hidden_ref.shape[0], chunk):
            natural = jnp.dot(
                restore_ref[n : n + chunk, :],
                attended_ref[...],
                preferred_element_type=jnp.float32,
            ).astype(jnp.bfloat16)
            projected = (
                jnp.dot(natural, w_ref[...], preferred_element_type=jnp.float32)
                + offset_ref[...]
            )
            centered = projected - jnp.mean(projected, axis=-1, keepdims=True)
            spread = jnp.mean(centered * centered, axis=-1, keepdims=True)
            normed = (
                centered * lax.rsqrt(spread + norm_epsilon) * gain_ref[...]
                + shift_ref[...]
            )
            result = (hidden_ref[n : n + chunk, :].astype(jnp.float32) + normed).astype(
                jnp.bfloat16
            )
            result = result.reshape(chunk // 16, 16, result.shape[-1])
            out_ref[n // 16 : (n + chunk) // 16] = result[:, : out_ref.shape[1], :]


def as_tiles(rows):
    main = rows[:, :128].reshape(72, 256)
    rest = np.pad(rows[:, 128:].reshape(2, 72, 16), ((0, 0), (0, 8), (0, 0))).reshape(10, 256)
    return np.concatenate([main, rest], axis=0)


def bias_constants():
    queries, keys = window_orders()
    eye = np.eye(WIN_TOK, dtype=np.float32)
    to_q = eye[queries]
    to_q_rest = np.pad(to_q.reshape(2, 72, WIN_TOK), ((0, 0), (0, 8), (0, 0)))
    to_q_rest = to_q_rest.reshape(160, WIN_TOK)
    to_k = eye[keys[:128]].T
    to_k_rest = eye[np.tile(keys[128:], 16)].T
    q_level, q_half = queries // 72, queries // 12 % 6 // 3
    k_level, k_row = keys // 72, keys // 12 % 6
    planes = [
        np.broadcast_to(k_row[None, :], (WIN_TOK, WIN_TOK)),
        q_half[:, None] == (k_row // 3)[None, :],
        q_level[:, None] == k_level[None, :],
    ]
    geometry = np.stack([as_tiles(p.astype(np.int32)) for p in planes], axis=1)
    matrices = [jnp.asarray(m, jnp.bfloat16) for m in (to_q, to_k, to_q_rest, to_k_rest)]
    return matrices + [jnp.asarray(geometry)]


def on_device(
    state_tokens,
    land_mask,
    pad_mask,
    land_embed,
    w_qkv,
    w_proj,
    proj_bias,
    norm_gain,
    norm_shift,
    bias_table,
    index_table,
):
    levels, lat_rows, lon_columns, features = state_tokens.shape
    assert (levels, lat_rows, lon_columns) == (2 * WIN_Z, 2 * WIN_LAT, WIN_LON)
    lat_total = lat_rows * lax.axis_size("lat")
    embedded = jnp.where(land_mask[:, :, None] == 1, land_embed[1], land_embed[0])
    hidden = (state_tokens.astype(jnp.float32) + embedded[None]).astype(jnp.bfloat16)
    hidden = jnp.pad(hidden, ((0, 0), (0, 0), (0, 16 - lon_columns), (0, 0)))
    hidden = hidden.reshape(levels * lat_rows * 16, features)
    rows = hidden.shape[0]
    placed, plain = token_orders(levels, lat_rows, lon_columns)
    natural = jnp.arange(rows, dtype=jnp.int32)
    to_groups = (jnp.asarray(placed)[:, None] == natural[None, :]).astype(jnp.bfloat16)
    restore = (natural[:, None] == jnp.asarray(plain)[None, :]).astype(jnp.bfloat16)
    grouped = jnp.dot(to_groups, hidden, preferred_element_type=jnp.float32).astype(jnp.bfloat16)
    shape = (2, 4, 2, SLOT)
    qkv = jnp.dot(grouped, w_qkv, preferred_element_type=jnp.float32)
    qkv = qkv.astype(jnp.bfloat16).reshape(2, 4, 2, SLOT, 3 * WIDTH)
    kv = qkv[..., WIDTH:]
    right = from_behind(kv[0], "lon", -1)
    left = from_behind(kv[1], "lon", 1)
    up = from_behind(jnp.stack([left[3], kv[0, 3], kv[1, 3], right[3]]), "lat", 1)
    down = from_behind(jnp.stack([left[0], kv[0, 0], kv[1, 0], right[0]]), "lat", -1)
    before = from_behind(bias_table[-1], "lat", 1)
    lat_index = lax.axis_index("lat").astype(jnp.int32).reshape(1)
    in_vmem = pl.BlockSpec(memory_space=pltpu.VMEM)
    in_smem = pl.BlockSpec(memory_space=pltpu.SMEM)
    highs = -(-bias_table.shape[-1] // LOW)
    bias = pl.pallas_call(
        bias_kernel,
        out_shape=jax.ShapeDtypeStruct((2, 2, 3, 36, 16, 256), jnp.bfloat16),
        in_specs=[in_vmem] * 3 + [in_smem] * 2 + [in_vmem] * 5,
        out_specs=in_vmem,
        scratch_shapes=[
            pltpu.VMEM((WIN_TOK + 32, 128), jnp.int32),
            pltpu.VMEM((WIN_TOK + 32, 128), jnp.int32),
            pltpu.VMEM((2, highs * 48, LOW), jnp.bfloat16),
        ],
        compiler_params=pltpu.CompilerParams(vmem_limit_bytes=24 << 20),
        cost_estimate=pl.CostEstimate(
            flops=2 * 82 * 624 * 256 * 256, bytes_accessed=8 << 20, transcendentals=0
        ),
        name="bias",
    )(index_table, before, bias_table, pad_mask, lat_index, *bias_constants())
    vectors = [v.reshape(1, features) for v in (proj_bias, norm_gain, norm_shift)]
    whole = pl.BlockSpec(memory_space=pltpu.VMEM)

    def bias_block(i):
        quarter, lon = i // 2, i % 2
        return (1 - quarter % 2, (quarter + 1) // 2 % 2, 0, 1 - lon, 0, 0)

    out = pl.pallas_call(
        attend_kernel,
        grid=(8,),
        out_shape=jax.ShapeDtypeStruct((levels * lat_rows, lon_columns, features), jnp.bfloat16),
        in_specs=[pl.BlockSpec((1, 1, 3, GROUP // 2, 16, 256), bias_block)] + [whole] * 11,
        out_specs=whole,
        scratch_shapes=[
            pltpu.VMEM((6, 2, WIN_TOK, 2 * WIDTH), jnp.bfloat16),
            pltpu.VMEM((rows, WIDTH), jnp.bfloat16),
        ],
        compiler_params=pltpu.CompilerParams(
            vmem_limit_bytes=40 << 20, dimension_semantics=("arbitrary",)
        ),
        name="attend",
    )(bias, qkv, left, right, up, down, hidden, restore, w_proj, *vectors)
    return out.reshape(state_tokens.shape)


def solution(mesh):
    in_specs = (
        P("member", "lat", "lon", None),
        P("lat", "lon"),
        P(),
        P(),
        P(),
        P(),
        P(),
        P(),
        P(),
        P("lat", None, None, None),
        P(),
    )
    out_specs = P("member", "lat", "lon", None)
    return jax.shard_map(
        on_device, mesh=mesh, in_specs=in_specs, out_specs=out_specs, check_vma=False
    )
```
